32 devices in a mesh: row: 8 (over y, x, core), col: 4 (over z).
Axes of the slice: x: 2, y: 2, z: 4, core: 2. Of those that a mesh axis runs over, the one named last changes fastest.
Arguments:
- jacobian: float32 [2, 4096, 256], P(None, ('row', 'col')), may hold values from -0.25 to 0.25
Outputs:
- normal_tiles: float32 [8, 2, 4, 512, 512], P('row', None, 'col')
The draws below stay inside these ranges and needn't reach their ends.
All inputs are finite; a program needn't handle non-finite values.
Results may differ from the reference program's by a relative error of at most 0.0003.
Values sent between devices are 32-bit elements; how exact they have to be, the bound alone decides.
No kernel may reach another device: no remote copies, remote signals or barrier semaphores. Data moves between devices by JAX's collectives and lax.ppermute only.
A program may use at most 64 MiB of HBM per device.

```python
import jax
import jax.numpy as jnp
from jax import lax

TILE = 512
KP = 256
PANELS = 2
NT = 8
CYC = 2
M = 4096
N_COL = 4


def block_levels(stream_key, shape, shards, smallest, largest):
    factor_of, own = 1.0, jax.random.fold_in(stream_key, 6)
    for dim, shards_of in shards:
        heights = jnp.exp(jax.random.uniform(jax.random.fold_in(own, dim), (shards_of,), jnp.float32, smallest / len(shards), largest / len(shards)))
        factor_of = factor_of * jnp.repeat(heights, shape[dim] // shards_of).reshape([-1 if axis == dim else 1 for axis in range(len(shape))])
    return factor_of


def gaussian(stream_key, dims, width, limit, pieces=(), kind=jnp.bfloat16):
    result = jax.random.normal(stream_key, dims, jnp.float32) * width
    if len(pieces) > 0:
        result = block_levels(stream_key, dims, pieces, -0.22, 0.18) * result
    return jnp.clip(result, min=-limit, max=limit).astype(kind)


def setup_inputs(seed: int = 0) -> dict:
    streams_of = jax.random.split(jax.random.key(seed), 2)
    jacobian = gaussian(streams_of[0], (PANELS, M, KP), (PANELS * KP) ** -0.5, 0.25, ((1, 32),), jnp.float32)
    return {"jacobian": jacobian}


def reference(jacobian):
    def one_row(index):
        row_block = lax.dynamic_slice_in_dim(jacobian, index * TILE, TILE, 1)
        products = jnp.einsum("pak,pbk->ab", row_block.astype(jnp.float32), jacobian.astype(jnp.float32), precision=lax.Precision.HIGHEST)
        arranged = products.reshape(TILE, CYC, N_COL, TILE).transpose(1, 2, 0, 3)
        column_tile = jnp.arange(CYC, dtype=jnp.int32)[:, None] * N_COL + jnp.arange(N_COL, dtype=jnp.int32)[None, :]
        keep_mask = column_tile <= index
        return jnp.where(keep_mask[:, :, None, None], arranged, jnp.zeros_like(arranged))
    return lax.map(one_row, jnp.arange(NT, dtype=jnp.int32))
```

```python
import jax
import jax.numpy as jnp
from jax import lax
from jax.experimental import pallas as pl
from jax.experimental.pallas import tpu as pltpu
from jax.sharding import PartitionSpec as P


def swap(block, bits):
    count = lax.axis_size("row")
    return lax.ppermute(block, "row", [(low, low ^ bits) for low in range(count)])


def shift(block, distance):
    count = lax.axis_size("col")
    return lax.ppermute(block, "col", [(low, (low + distance) % count) for low in range(count)])


def transposed(block, skew):
    rows, cols = lax.axis_size("row"), lax.axis_size("col")
    route = []
    for row in range(rows):
        for col in range(cols):
            target = row // cols * cols + (col + skew) % cols
            route.append((row * cols + col, target * cols + row % cols))
    return lax.ppermute(block, ("row", "col"), route)


def body(jacobian):
    rows, cols = lax.axis_size("row"), lax.axis_size("col")
    cycles = rows // cols
    panels, depth, width = jacobian.shape
    tile = depth * cols
    half = panels // 2
    skew = cols // 2
    moved = [transposed(jacobian[:half], 0), transposed(jacobian[half:], skew)]
    near = [shift(jacobian, distance) for distance in range(1, cols)]
    bits = [1 << number for number in range(rows.bit_length() - 1)]
    first, second = bits[1], bits[2]
    low, high = moved
    low_first, high_first = swap(low, first), swap(high, first)
    low_second, high_second = swap(low, second), swap(high, second)
    low_far, high_far = swap(low_first, second), swap(high_second, first)
    held = [
        (0, 0, low), (0, 1, high),
        (first, 0, low_first), (first, 1, high_first),
        (second, 0, low_second), (second, 1, high_second),
        (first | second, 0, low_far), (first | second, 1, high_far),
    ]
    for bit in bits[:1] + bits[3:]:
        held += [(distance ^ bit, part, swap(block, bit)) for distance, part, block in held]
    pieces = [block for _, _, block in held]
    kinds = [(distance, part) for distance, part, _ in held]

    def kernel(position, own, *refs):
        shifted = refs[: cols - 1]
        columns = refs[cols - 1 : cols - 1 + len(pieces)]
        out, row_hi, row_lo, col_hi, col_lo = refs[cols - 1 + len(pieces) :]
        row_index, col_index = position[0], position[1]

        def split(value, hi, lo, lead, start, lane):
            top = value.astype(jnp.bfloat16)
            rest = (value - top.astype(jnp.float32)).astype(jnp.bfloat16)
            where = pl.ds(pl.multiple_of(start, depth), depth)
            hi[lead, where, lane * width : (lane + 1) * width] = top
            lo[lead, where, lane * width : (lane + 1) * width] = rest

        for distance, source in enumerate((own,) + tuple(shifted)):
            start = lax.rem(col_index - distance + cols, cols) * depth
            for panel in range(panels):
                split(source[panel], row_hi, row_lo, 0, start, panel)
        for (distance, part), source in zip(kinds, columns):
            holder = row_index ^ distance
            turn = holder // cols
            slot = lax.rem(holder - turn * cols - part * skew + cols, cols)
            for panel in range(half):
                split(source[panel], col_hi, col_lo, turn, slot * depth, part * half + panel)

        def dot(left, right):
            return lax.dot_general(
                left, right, (((1,), (1,)), ((), ())), preferred_element_type=jnp.float32
            )

        for turn in range(cycles):
            wanted = turn * cols + col_index <= row_index

            @pl.when(wanted)
            def _():
                out[0, turn, 0] = (
                    dot(row_hi[0], col_lo[turn]) + dot(row_lo[0], col_hi[turn])
                ) + dot(row_hi[0], col_hi[turn])

            @pl.when(jnp.logical_not(wanted))
            def _():
                out[0, turn, 0] = jnp.zeros((tile, tile), jnp.float32)

    position = jnp.stack([lax.axis_index("row"), lax.axis_index("col")]).astype(jnp.int32)
    vmem = pl.BlockSpec(memory_space=pltpu.VMEM)
    return pl.pallas_call(
        kernel,
        out_shape=jax.ShapeDtypeStruct((1, cycles, 1, tile, tile), jnp.float32),
        in_specs=[pl.BlockSpec(memory_space=pltpu.SMEM)] + [vmem] * (cols + len(pieces)),
        out_specs=vmem,
        scratch_shapes=[
            pltpu.VMEM((1, tile, panels * width), jnp.bfloat16),
            pltpu.VMEM((1, tile, panels * width), jnp.bfloat16),
            pltpu.VMEM((cycles, tile, panels * width), jnp.bfloat16),
            pltpu.VMEM((cycles, tile, panels * width), jnp.bfloat16),
        ],
        compiler_params=pltpu.CompilerParams(vmem_limit_bytes=24 << 20),
        cost_estimate=pl.CostEstimate(
            flops=6 * cycles * tile * tile * panels * width,
            bytes_accessed=4 * cycles * tile * tile * 2,
            transcendentals=0,
        ),
    )(position, jacobian, *near, *pieces)


def solution(mesh):
    in_specs = (P(None, ("row", "col"), None),)
    out_specs = P("row", None, "col", None, None)
    return jax.shard_map(body, mesh=mesh, in_specs=in_specs, out_specs=out_specs, check_vma=False)
```

```python
import jax
import jax.numpy as jnp
from jax import lax
from jax.experimental import pallas as pl
from jax.experimental.pallas import tpu as pltpu
from jax.sharding import PartitionSpec as P


def swap(block, bits):
    count = lax.axis_size("row")
    return lax.ppermute(block, "row", [(low, low ^ bits) for low in range(count)])


def shift(block, distance):
    rows, cols = lax.axis_size("row"), lax.axis_size("col")
    route = []
    for row in range(rows):
        for col in range(cols):
            target = (col + distance) % cols
            if target < row and row % cols != target:
                route.append((row * cols + col, row * cols + target))
    return lax.ppermute(block, ("row", "col"), route)


def transpose(block):
    rows, cols = lax.axis_size("row"), lax.axis_size("col")
    route = []
    for row in range(rows):
        for col in range(cols):
            target = row // cols * cols + col
            route.append((row * cols + col, target * cols + row % cols))
    return lax.ppermute(block, ("row", "col"), route)


def tiles(jacobian):
    rows, cols = lax.axis_size("row"), lax.axis_size("col")
    cycles = rows // cols
    panels, depth, width = jacobian.shape
    tile = depth * cols
    half = panels // 2
    moved = transpose(jacobian)
    near = [shift(jacobian, distance) for distance in range(1, cols)]
    bits = [1 << number for number in range(rows.bit_length() - 1)]
    first, second = bits[1], bits[2]
    by_first = swap(moved, first)
    by_second = swap(moved, second)
    low_far = swap(by_first[:half], second)
    high_far = swap(by_second[half:], first)
    held = [
        (0, 0, moved), (first, 0, by_first), (second, 0, by_second),
        (first | second, 0, low_far), (first | second, half, high_far),
    ]
    for bit in bits[:1] + bits[3:]:
        held += [
            (distance ^ bit, panel, swap(block, bit))
            for distance, panel, block in held
        ]
    pieces = [block for _, _, block in held]
    kinds = [(distance, panel) for distance, panel, _ in held]

    spread = panels * width
    vmem = pl.BlockSpec(memory_space=pltpu.VMEM)
    smem = pl.BlockSpec(memory_space=pltpu.SMEM)

    def split(value, hi, lo, lead, start, panel):
        top = value.astype(jnp.bfloat16)
        where = pl.ds(pl.multiple_of(start, depth), depth)
        hi[lead, where, panel * width : (panel + 1) * width] = top
        lo[lead, where, panel * width : (panel + 1) * width] = (
            value - top.astype(jnp.float32)
        ).astype(jnp.bfloat16)

    def split_columns(position, *refs):
        columns, (hi, lo) = refs[: len(pieces)], refs[len(pieces) :]
        for (distance, lead), source in zip(kinds, columns):
            holder = position[0] ^ distance
            turn = holder // cols
            for panel in range(source.shape[0]):
                split(source[panel], hi, lo, turn, (holder - turn * cols) * depth, lead + panel)

    def multiply(position, own, *refs):
        blocks = (own,) + tuple(refs[: cols - 1])
        col_hi, col_lo, out, row_hi, row_lo, stage, sems = refs[cols - 1 :]
        row_index, col_index = position[0], position[1]
        own_turn = row_index // cols
        diagonal = row_index - own_turn * cols == col_index

        @pl.when(diagonal)
        def _():
            row_hi[0] = col_hi[own_turn]
            row_lo[0] = col_lo[own_turn]

        @pl.when(jnp.logical_not(diagonal))
        def _():
            for distance, source in enumerate(blocks):
                start = lax.rem(col_index - distance + cols, cols) * depth
                for panel in range(panels):
                    split(source[panel], row_hi, row_lo, 0, start, panel)

        def dot(left, right):
            return lax.dot_general(
                left, right, (((1,), (1,)), ((), ())), preferred_element_type=jnp.float32
            )

        copies = []
        for turn in range(cycles):
            wanted = turn * cols + col_index <= row_index

            @pl.when(wanted)
            def _():
                stage[turn] = (
                    dot(row_hi[0], col_lo[turn]) + dot(row_lo[0], col_hi[turn])
                ) + dot(row_hi[0], col_hi[turn])

            @pl.when(jnp.logical_not(wanted))
            def _():
                stage[turn] = jnp.zeros((tile, tile), jnp.float32)

            copies.append(pltpu.make_async_copy(stage.at[turn], out.at[0, turn, 0], sems.at[turn]))
            copies[-1].start()
        for copy in copies:
            copy.wait()

    position = jnp.stack([lax.axis_index("row"), lax.axis_index("col")]).astype(jnp.int32)
    halves = jax.ShapeDtypeStruct((cycles, tile, spread), jnp.bfloat16)
    col_hi, col_lo = pl.pallas_call(
        split_columns,
        out_shape=(halves, halves),
        in_specs=[smem] + [vmem] * len(pieces),
        out_specs=(vmem, vmem),
        compiler_params=pltpu.CompilerParams(vmem_limit_bytes=16 << 20),
        cost_estimate=pl.CostEstimate(
            flops=8 * cycles * tile * spread,
            bytes_accessed=8 * cycles * tile * spread,
            transcendentals=0,
        ),
    )(position, *pieces)
    return pl.pallas_call(
        multiply,
        out_shape=jax.ShapeDtypeStruct((1, cycles, 1, tile, tile), jnp.float32),
        in_specs=[smem] + [vmem] * (cols + 2),
        out_specs=pl.BlockSpec(memory_space=pl.ANY),
        scratch_shapes=[
            pltpu.VMEM((1, tile, spread), jnp.bfloat16),
            pltpu.VMEM((1, tile, spread), jnp.bfloat16),
            pltpu.VMEM((cycles, tile, tile), jnp.float32),
            pltpu.SemaphoreType.DMA((cycles,)),
        ],
        compiler_params=pltpu.CompilerParams(vmem_limit_bytes=24 << 20),
        cost_estimate=pl.CostEstimate(
            flops=6 * cycles * tile * tile * spread,
            bytes_accessed=8 * cycles * tile * tile,
            transcendentals=0,
        ),
    )(position, jacobian, *near, col_hi, col_lo)


def solution(mesh):
    in_specs = (P(None, ("row", "col"), None),)
    out_specs = P("row", None, "col", None, None)
    return jax.shard_map(tiles, mesh=mesh, in_specs=in_specs, out_specs=out_specs, check_vma=False)
```

```python
import jax
import jax.numpy as jnp
from jax import lax
from jax.experimental import pallas as pl
from jax.experimental.pallas import tpu as pltpu
from jax.sharding import PartitionSpec as P


def swap(block, bits):
    count = lax.axis_size("row")
    route = [(low, low ^ bits) for low in range(count)]
    return lax.ppermute(block, "row", route)


def sense(row, cols):
    return 1 if row % cols < cols // 2 else -1


def reads(row, col, cols):
    return col < row and row % cols != col


def shift(block, distance):
    rows, cols = lax.axis_size("row"), lax.axis_size("col")
    route = []
    for row in range(rows):
        for col in range(cols):
            place = col + sense(row, cols) * distance
            if reads(row, place % cols, cols):
                route.append((row * cols + col, row * cols + place % cols))
    return lax.ppermute(block, ("row", "col"), route)


def transpose(block):
    rows, cols = lax.axis_size("row"), lax.axis_size("col")
    route = []
    for row in range(rows):
        for col in range(cols):
            target = row // cols * cols + (col + cols // 2) % cols
            route.append((row * cols + col, target * cols + row % cols))
    return lax.ppermute(block, ("row", "col"), route)


def row_bits(rows):
    bits = [1 << number for number in range(1, rows.bit_length() - 1)]
    distances = [0]
    for bit in bits:
        distances += [distance | bit for distance in distances]
    return distances[1:2] + distances[:1:-1], 1


def tiles(jacobian):
    rows, cols = lax.axis_size("row"), lax.axis_size("col")
    cycles = rows // cols
    panels, depth, width = jacobian.shape
    tile = depth * cols
    half = panels // 2
    first = jacobian[:half]
    parts = (first, lax.optimization_barrier((jacobian, first))[0][half:])
    moved = [transpose(part) for part in parts]
    near = [shift(jacobian, distance) for distance in range(1, cols)]
    far, twin = row_bits(rows)
    held = []
    for part in moved:
        pieces = {0: part}
        for distance in far:
            pieces[distance] = swap(part, distance)
        for distance in [0] + far:
            pieces[distance ^ twin] = swap(pieces[distance], twin)
        held.append(pieces)
    vmem = pl.BlockSpec(memory_space=pltpu.VMEM)
    smem = pl.BlockSpec(memory_space=pltpu.SMEM)
    params = pltpu.CompilerParams(vmem_limit_bytes=16 << 20)
    lanes = half * width
    position = jnp.stack([lax.axis_index("row"), lax.axis_index("col")]).astype(jnp.int32)

    def split(value, hi, lo, lead, start, panel):
        top = value.astype(jnp.bfloat16)
        where = (lead, pl.ds(pl.multiple_of(start, depth), depth), slice(panel * width, (panel + 1) * width))
        hi[where] = top
        lo[where] = (value - top.astype(jnp.float32)).astype(jnp.bfloat16)

    def split_columns(position, *refs):
        pieces, (hi, lo) = refs[:rows], refs[rows:]
        for distance, source in enumerate(pieces):
            holder = position[0] ^ distance
            turn = holder // cols
            slot = lax.rem(holder - turn * cols + cols - cols // 2, cols)
            for panel in range(half):
                split(source[panel], hi, lo, turn, slot * depth, panel)

    def columns(pieces):
        shape = jax.ShapeDtypeStruct((cycles, tile, lanes), jnp.bfloat16)
        return pl.pallas_call(
            split_columns,
            out_shape=(shape, shape),
            in_specs=[smem] + [vmem] * rows,
            out_specs=(vmem, vmem),
            compiler_params=params,
            cost_estimate=pl.CostEstimate(
                flops=4 * cycles * tile * lanes, bytes_accessed=8 * cycles * tile * lanes, transcendentals=0
            ),
        )(position, *[pieces[distance] for distance in range(rows)])

    split_parts = [columns(pieces) for pieces in held]

    chunks = 2
    chunk = tile // chunks

    def dot(left, right):
        return lax.dot_general(
            left, right, (((1,), (1,)), ((), ())), preferred_element_type=jnp.float32
        )

    def multiply(position, *refs):
        own, blocks, refs = refs[:2], refs[2 : cols + 1], refs[cols + 1 :]
        col_hi, col_lo = (refs[0], refs[2]), (refs[1], refs[3])
        out, row_hi, row_lo, stage, sems = refs[4:]
        row, col = position[0], position[1]
        own_turn = row // cols
        diagonal = row - own_turn * cols == col

        def copy(turn, part):
            where = slice(part * chunk, (part + 1) * chunk)
            return pltpu.make_async_copy(
                stage.at[turn, :, where], out.at[0, turn, 0, :, where], sems.at[turn, part]
            )

        wanted = [turn * cols + col <= row for turn in range(cycles)]
        for turn in range(cycles):

            @pl.when(jnp.logical_not(wanted[turn]))
            def _():
                stage[turn] = jnp.zeros((tile, tile), jnp.float32)
                for part in range(chunks):
                    copy(turn, part).start()

        @pl.when(diagonal)
        def _():
            for part in range(2):
                row_hi[part] = col_hi[part][own_turn]
                row_lo[part] = col_lo[part][own_turn]

        @pl.when(jnp.logical_not(diagonal))
        def _():
            ahead = lax.rem(row, cols) < cols // 2
            for distance in range(cols):
                back = jnp.where(ahead, cols - distance, distance)
                start = lax.rem(col + back, cols) * depth
                for panel in range(panels):
                    source = blocks[distance - 1][panel] if distance else own[panel // half][panel % half]
                    split(source, row_hi, row_lo, panel // half, start, panel % half)

        for turn in range(cycles):

            @pl.when(wanted[turn])
            def _():
                for number in range(chunks):
                    where = slice(number * chunk, (number + 1) * chunk)
                    total = None
                    for part in range(2):
                        hi, lo = col_hi[part][turn, where], col_lo[part][turn, where]
                        term = dot(row_hi[part], lo) + dot(row_lo[part], hi) + dot(row_hi[part], hi)
                        total = term if total is None else total + term
                    stage[turn, :, where] = total
                    copy(turn, number).start()

        for turn in range(cycles):
            for part in range(chunks):
                copy(turn, part).wait()

    half_rows = pltpu.VMEM((2, tile, lanes), jnp.bfloat16)
    return pl.pallas_call(
        multiply,
        out_shape=jax.ShapeDtypeStruct((1, cycles, 1, tile, tile), jnp.float32),
        in_specs=[smem] + [vmem] * (cols + 5),
        out_specs=pl.BlockSpec(memory_space=pl.ANY),
        scratch_shapes=[
            half_rows,
            half_rows,
            pltpu.VMEM((cycles, tile, tile), jnp.float32),
            pltpu.SemaphoreType.DMA((cycles, chunks)),
        ],
        compiler_params=params,
        cost_estimate=pl.CostEstimate(
            flops=6 * cycles * tile * tile * panels * width,
            bytes_accessed=8 * cycles * tile * tile,
            transcendentals=0,
        ),
    )(position, *parts, *near, *split_parts[0], *split_parts[1])


def solution(mesh):
    in_specs = (P(None, ("row", "col"), None),)
    out_specs = P("row", None, "col", None, None)
    return jax.shard_map(tiles, mesh=mesh, in_specs=in_specs, out_specs=out_specs, check_vma=False)
```

```python
import jax
import jax.numpy as jnp
from jax import lax
from jax.experimental import pallas as pl
from jax.experimental.pallas import tpu as pltpu
from jax.sharding import PartitionSpec as P


ROW_ORDER, COL_ORDER = ("hi", "lo"), ("lo", "hi")


def swap(block, bits):
    count = lax.axis_size("row")
    route = [(low, low ^ bits) for low in range(count)]
    return lax.ppermute(block, "row", route)


def sense(row, cols):
    return 1 if row % cols < cols // 2 else -1


def reads(row, col, cols):
    return col < row and row % cols != col


def shift(block, distance, straight):
    rows, cols = lax.axis_size("row"), lax.axis_size("col")
    route = []
    for row in range(rows):
        for col in range(cols):
            place = col + sense(row, cols) * distance
            inside = 0 <= place < cols
            if straight in (None, inside) and reads(row, place % cols, cols):
                route.append((row * cols + col, row * cols + place % cols))
    return lax.ppermute(block, ("row", "col"), route)


def transpose(block):
    rows, cols = lax.axis_size("row"), lax.axis_size("col")
    route = []
    for row in range(rows):
        for col in range(cols):
            target = row // cols * cols + (col + cols // 2) % cols
            route.append((row * cols + col, target * cols + row % cols))
    return lax.ppermute(block, ("row", "col"), route)


def row_bits(rows):
    bits = [1 << number for number in range(1, rows.bit_length() - 1)]
    distances = [0]
    for bit in bits:
        distances += [distance | bit for distance in distances]
    return distances[:0:-1], 1


def tiles(jacobian):
    rows, cols = lax.axis_size("row"), lax.axis_size("col")
    cycles = rows // cols
    panels, depth, width = jacobian.shape
    tile = depth * cols
    half = panels // 2
    first = jacobian[:half]
    parts = (first, lax.optimization_barrier((jacobian, first))[0][half:])
    moved = [transpose(part) for part in parts]
    halved = range(2, cols - 1)
    near = [shift(jacobian, distance, True if distance in halved else None) for distance in range(1, cols)]
    near += [shift(jacobian, distance, False) for distance in halved]
    far, twin = row_bits(rows)
    held = []
    for part in moved:
        pieces = {0: part}
        for distance in far:
            pieces[distance] = swap(part, distance)
        for distance in [0] + far:
            pieces[distance ^ twin] = swap(pieces[distance], twin)
        held.append(pieces)
    vmem = pl.BlockSpec(memory_space=pltpu.VMEM)
    smem = pl.BlockSpec(memory_space=pltpu.SMEM)
    params = pltpu.CompilerParams(vmem_limit_bytes=16 << 20)
    lanes = half * width
    position = jnp.stack([lax.axis_index("row"), lax.axis_index("col")]).astype(jnp.int32)

    def split(value, parts, order, lead, start, panel):
        top = value.astype(jnp.bfloat16)
        rest = (value - top.astype(jnp.float32)).astype(jnp.bfloat16)
        where = pl.ds(pl.multiple_of(start, depth), depth)
        for place, kind in enumerate(order):
            first = place * lanes + panel * width
            parts[lead, where, first : first + width] = top if kind == "hi" else rest

    def split_columns(position, *refs):
        pieces, whole = refs[:rows], refs[rows]
        for distance, source in enumerate(pieces):
            holder = position[0] ^ distance
            turn = holder // cols
            slot = lax.rem(holder - turn * cols + cols - cols // 2, cols)
            for panel in range(half):
                split(source[panel], whole, COL_ORDER, turn, slot * depth, panel)

    def columns(pieces):
        shape = jax.ShapeDtypeStruct((cycles, tile, len(COL_ORDER) * lanes), jnp.bfloat16)
        return pl.pallas_call(
            split_columns,
            out_shape=shape,
            in_specs=[smem] + [vmem] * rows,
            out_specs=vmem,
            compiler_params=params,
            cost_estimate=pl.CostEstimate(
                flops=4 * cycles * tile * lanes, bytes_accessed=8 * cycles * tile * lanes, transcendentals=0
            ),
        )(position, *[pieces[distance] for distance in range(rows)])

    split_parts = [columns(pieces) for pieces in held]

    chunks = 1
    chunk = tile // chunks

    def dot(left, right):
        return lax.dot_general(
            left, right, (((1,), (1,)), ((), ())), preferred_element_type=jnp.float32
        )

    def multiply(position, *refs):
        own, blocks, refs = refs[:2], refs[2 : 2 + len(near)], refs[2 + len(near) :]
        columns_of = refs[:2]
        out, rows_of, stage, sems = refs[2:]
        row, col = position[0], position[1]
        own_turn = row // cols
        diagonal = row - own_turn * cols == col

        def copy(turn, part):
            where = slice(part * chunk, (part + 1) * chunk)
            return pltpu.make_async_copy(
                stage.at[turn, :, where], out.at[0, turn, 0, :, where], sems.at[turn, part]
            )

        wanted = [turn * cols + col <= row for turn in range(cycles)]
        for turn in range(cycles):

            @pl.when(jnp.logical_not(wanted[turn]))
            def _():
                stage[turn] = jnp.zeros((tile, tile), jnp.float32)
                for part in range(chunks):
                    copy(turn, part).start()

        @pl.when(diagonal)
        def _():
            for part in range(2):
                for place, kind in enumerate(ROW_ORDER):
                    first = COL_ORDER.index(kind) * lanes
                    rows_of[part, :, place * lanes : (place + 1) * lanes] = columns_of[part][
                        own_turn, :, first : first + lanes
                    ]

        @pl.when(jnp.logical_not(diagonal))
        def _():
            ahead = lax.rem(row, cols) < cols // 2
            for distance in range(cols):
                back = jnp.where(ahead, cols - distance, distance)
                start = lax.rem(col + back, cols) * depth
                for panel in range(panels):
                    source = blocks[distance - 1][panel] if distance else own[panel // half][panel % half]
                    if distance in halved:
                        source += blocks[cols - 3 + distance][panel]
                    split(source, rows_of, ROW_ORDER, panel // half, start, panel % half)

        for turn in range(cycles):

            @pl.when(wanted[turn])
            def _():
                for number in range(chunks):
                    where = slice(number * chunk, (number + 1) * chunk)
                    total = None
                    for part in range(2):
                        term = dot(rows_of[part], columns_of[part][turn, where])
                        term += dot(rows_of[part, :, :lanes], columns_of[part][turn, where, lanes:])
                        total = term if total is None else total + term
                    stage[turn, :, where] = total
                    copy(turn, number).start()

        for turn in range(cycles):
            for part in range(chunks):
                copy(turn, part).wait()

    half_rows = pltpu.VMEM((2, tile, len(ROW_ORDER) * lanes), jnp.bfloat16)
    return pl.pallas_call(
        multiply,
        out_shape=jax.ShapeDtypeStruct((1, cycles, 1, tile, tile), jnp.float32),
        in_specs=[smem] + [vmem] * (len(near) + 4),
        out_specs=pl.BlockSpec(memory_space=pl.ANY),
        scratch_shapes=[
            half_rows,
            pltpu.VMEM((cycles, tile, tile), jnp.float32),
            pltpu.SemaphoreType.DMA((cycles, chunks)),
        ],
        compiler_params=params,
        cost_estimate=pl.CostEstimate(
            flops=6 * cycles * tile * tile * panels * width,
            bytes_accessed=8 * cycles * tile * tile,
            transcendentals=0,
        ),
    )(position, *parts, *near, *split_parts)


def solution(mesh):
    in_specs = (P(None, ("row", "col"), None),)
    out_specs = P("row", None, "col", None, None)
    return jax.shard_map(tiles, mesh=mesh, in_specs=in_specs, out_specs=out_specs, check_vma=False)
```

```python
import jax
import jax.numpy as jnp
from jax import lax
from jax.experimental import pallas as pl
from jax.experimental.pallas import tpu as pltpu
from jax.sharding import PartitionSpec as P


ROW_ORDER, COL_ORDER = ("hi", "lo"), ("lo", "hi")


def swap(block, bits):
    count = lax.axis_size("row")
    route = [(low, low ^ bits) for low in range(count)]
    return lax.ppermute(block, "row", route)


def sense(row, cols):
    return 1 if row % cols < cols // 2 else -1


def reads(row, col, cols):
    return col < row and row % cols != col


def shift(block, distance, straight):
    rows, cols = lax.axis_size("row"), lax.axis_size("col")
    route = []
    for row in range(rows):
        for col in range(cols):
            place = col + sense(row, cols) * distance
            inside = 0 <= place < cols
            if straight in (None, inside) and (straight or reads(row, place % cols, cols)):
                route.append((row * cols + col, row * cols + place % cols))
    return lax.ppermute(block, ("row", "col"), route)


def transpose(block):
    rows, cols = lax.axis_size("row"), lax.axis_size("col")
    route = []
    for row in range(rows):
        for col in range(cols):
            target = row // cols * cols + (col + cols // 2) % cols
            route.append((row * cols + col, target * cols + row % cols))
    return lax.ppermute(block, ("row", "col"), route)


def row_bits(rows):
    bits = [1 << number for number in range(1, rows.bit_length() - 1)]
    distances = [0]
    for bit in bits:
        distances += [distance | bit for distance in distances]
    return distances[:0:-1], 1


def tiles(jacobian):
    rows, cols = lax.axis_size("row"), lax.axis_size("col")
    cycles = rows // cols
    panels, depth, width = jacobian.shape
    tile = depth * cols
    half = panels // 2
    parts = (jacobian[:half], jacobian[half:])
    moved = [transpose(part) for part in parts]
    halved = range(2, cols - 1)
    near = [shift(jacobian, distance, True if distance in halved else None) for distance in range(1, cols)]
    near += [shift(jacobian, distance, False) for distance in halved]
    far, twin = row_bits(rows)
    held = []
    for part in moved:
        pieces = {0: part}
        for distance in far:
            pieces[distance] = swap(part, distance)
        for distance in [0] + far:
            pieces[distance ^ twin] = swap(pieces[distance], twin)
        held.append(pieces)
    vmem = pl.BlockSpec(memory_space=pltpu.VMEM)
    smem = pl.BlockSpec(memory_space=pltpu.SMEM)
    params = pltpu.CompilerParams(vmem_limit_bytes=16 << 20)
    lanes = half * width
    position = jnp.stack([lax.axis_index("row"), lax.axis_index("col")]).astype(jnp.int32)

    def split(value, parts, order, lead, start, panel):
        top = value.astype(jnp.bfloat16)
        rest = (value - top.astype(jnp.float32)).astype(jnp.bfloat16)
        where = pl.ds(pl.multiple_of(start, depth), depth)
        for place, kind in enumerate(order):
            first = place * lanes + panel * width
            parts[lead, where, first : first + width] = top if kind == "hi" else rest

    def split_columns(position, *refs):
        pieces, whole = refs[:rows], refs[rows]
        for distance, source in enumerate(pieces):
            holder = position[0] ^ distance
            turn = holder // cols
            slot = lax.rem(holder - turn * cols + cols - cols // 2, cols)
            for panel in range(half):
                split(source[panel], whole, COL_ORDER, turn, slot * depth, panel)

    def columns(pieces):
        shape = jax.ShapeDtypeStruct((cycles, tile, len(COL_ORDER) * lanes), jnp.bfloat16)
        return pl.pallas_call(
            split_columns,
            out_shape=shape,
            in_specs=[smem] + [vmem] * rows,
            out_specs=vmem,
            compiler_params=params,
            cost_estimate=pl.CostEstimate(
                flops=4 * cycles * tile * lanes, bytes_accessed=8 * cycles * tile * lanes, transcendentals=0
            ),
        )(position, *[pieces[distance] for distance in range(rows)])

    split_parts = [columns(pieces) for pieces in held]

    chunks = 1
    chunk = tile // chunks

    def dot(left, right):
        return lax.dot_general(
            left, right, (((1,), (1,)), ((), ())), preferred_element_type=jnp.float32
        )

    def multiply(position, *refs):
        own, blocks, refs = refs[:2], refs[2 : 2 + len(near)], refs[2 + len(near) :]
        columns_of = refs[:2]
        out, rows_of, stage, sems = refs[2:]
        row, col = position[0], position[1]
        own_turn = row // cols
        diagonal = row - own_turn * cols == col

        def copy(turn, part):
            where = slice(part * chunk, (part + 1) * chunk)
            return pltpu.make_async_copy(
                stage.at[turn, :, where], out.at[0, turn, 0, :, where], sems.at[turn, part]
            )

        wanted = [turn * cols + col <= row for turn in range(cycles)]
        for turn in range(cycles):

            @pl.when(jnp.logical_not(wanted[turn]))
            def _():
                stage[turn] = jnp.zeros((tile, tile), jnp.float32)
                for part in range(chunks):
                    copy(turn, part).start()

        @pl.when(diagonal)
        def _():
            for part in range(2):
                for place, kind in enumerate(ROW_ORDER):
                    first = COL_ORDER.index(kind) * lanes
                    rows_of[part, :, place * lanes : (place + 1) * lanes] = columns_of[part][
                        own_turn, :, first : first + lanes
                    ]

        @pl.when(jnp.logical_not(diagonal))
        def _():
            ahead = lax.rem(row, cols) < cols // 2
            for distance in range(cols):
                back = jnp.where(ahead, cols - distance, distance)
                start = lax.rem(col + back, cols) * depth
                for panel in range(panels):
                    source = blocks[distance - 1][panel] if distance else own[panel // half][panel % half]
                    if distance in halved:
                        source += blocks[cols - 3 + distance][panel]
                    split(source, rows_of, ROW_ORDER, panel // half, start, panel % half)

        for turn in range(cycles):

            @pl.when(wanted[turn])
            def _():
                for number in range(chunks):
                    where = slice(number * chunk, (number + 1) * chunk)
                    total = None
                    for part in range(2):
                        term = dot(rows_of[part], columns_of[part][turn, where])
                        term += dot(rows_of[part, :, :lanes], columns_of[part][turn, where, lanes:])
                        total = term if total is None else total + term
                    stage[turn, :, where] = total
                    copy(turn, number).start()

        for turn in range(cycles):
            for part in range(chunks):
                copy(turn, part).wait()

    half_rows = pltpu.VMEM((2, tile, len(ROW_ORDER) * lanes), jnp.bfloat16)
    return pl.pallas_call(
        multiply,
        out_shape=jax.ShapeDtypeStruct((1, cycles, 1, tile, tile), jnp.float32),
        in_specs=[smem] + [vmem] * (len(near) + 4),
        out_specs=pl.BlockSpec(memory_space=pl.ANY),
        scratch_shapes=[
            half_rows,
            pltpu.VMEM((cycles, tile, tile), jnp.float32),
            pltpu.SemaphoreType.DMA((cycles, chunks)),
        ],
        compiler_params=params,
        cost_estimate=pl.CostEstimate(
            flops=6 * cycles * tile * tile * panels * width,
            bytes_accessed=8 * cycles * tile * tile,
            transcendentals=0,
        ),
    )(position, *parts, *near, *split_parts)


def solution(mesh):
    in_specs = (P(None, ("row", "col"), None),)
    out_specs = P("row", None, "col", None, None)
    return jax.shard_map(tiles, mesh=mesh, in_specs=in_specs, out_specs=out_specs, check_vma=False)
```

```python
import jax
import jax.numpy as jnp
from jax import lax
from jax.experimental import pallas as pl
from jax.experimental.pallas import tpu as pltpu
from jax.sharding import PartitionSpec as P


ROW_ORDER, COL_ORDER = ("hi", "lo"), ("lo", "hi")


def swap(block, bits):
    count = lax.axis_size("row")
    route = [(low, low ^ bits) for low in range(count)]
    return lax.ppermute(block, "row", route)


def sense(row, cols):
    return 1 if row % cols < cols // 2 else -1


def reads(row, col, cols):
    return col < row and row % cols != col


def shift(block, distance, straight):
    rows, cols = lax.axis_size("row"), lax.axis_size("col")
    route = []
    for row in range(rows):
        for col in range(cols):
            place = col + sense(row, cols) * distance
            inside = 0 <= place < cols
            if straight in (None, inside) and (straight or reads(row, place % cols, cols)):
                route.append((row * cols + col, row * cols + place % cols))
    return lax.ppermute(block, ("row", "col"), route)


def transpose(block):
    rows, cols = lax.axis_size("row"), lax.axis_size("col")
    route = []
    for row in range(rows):
        for col in range(cols):
            target = row // cols * cols + (col + cols // 2) % cols
            route.append((row * cols + col, target * cols + row % cols))
    return lax.ppermute(block, ("row", "col"), route)


def row_bits(rows):
    bits = [1 << number for number in range(1, rows.bit_length() - 1)]
    distances = [0]
    for bit in bits:
        distances += [distance | bit for distance in distances]
    return distances[len(distances) // 2 :] + distances[1 : len(distances) // 2], 1


def tiles(jacobian):
    rows, cols = lax.axis_size("row"), lax.axis_size("col")
    cycles = rows // cols
    panels, depth, width = jacobian.shape
    tile = depth * cols
    half = panels // 2
    parts = (jacobian[:half], jacobian[half:])
    moved = [transpose(part) for part in parts]
    halved = range(2, cols - 1)
    near = [shift(jacobian, distance, True if distance in halved else None) for distance in range(1, cols)]
    near += [shift(jacobian, distance, False) for distance in halved]
    far, twin = row_bits(rows)
    held = []
    for part in moved:
        pieces = {0: part}
        for distance in far:
            pieces[distance] = swap(part, distance)
        for distance in [0] + far:
            pieces[distance ^ twin] = swap(pieces[distance], twin)
        held.append(pieces)
    vmem = pl.BlockSpec(memory_space=pltpu.VMEM)
    smem = pl.BlockSpec(memory_space=pltpu.SMEM)
    params = pltpu.CompilerParams(vmem_limit_bytes=16 << 20)
    lanes = half * width
    position = jnp.stack([lax.axis_index("row"), lax.axis_index("col")]).astype(jnp.int32)

    def split(value, parts, order, lead, start, panel):
        top = value.astype(jnp.bfloat16)
        rest = (value - top.astype(jnp.float32)).astype(jnp.bfloat16)
        where = pl.ds(pl.multiple_of(start, depth), depth)
        for place, kind in enumerate(order):
            first = place * lanes + panel * width
            parts[lead, where, first : first + width] = top if kind == "hi" else rest

    def split_columns(position, *refs):
        pieces, whole = refs[:rows], refs[rows]
        for distance, source in enumerate(pieces):
            holder = position[0] ^ distance
            turn = holder // cols
            slot = lax.rem(holder - turn * cols + cols - cols // 2, cols)
            for panel in range(half):
                split(source[panel], whole, COL_ORDER, turn, slot * depth, panel)

    def columns(pieces):
        shape = jax.ShapeDtypeStruct((cycles, tile, len(COL_ORDER) * lanes), jnp.bfloat16)
        return pl.pallas_call(
            split_columns,
            out_shape=shape,
            in_specs=[smem] + [vmem] * rows,
            out_specs=vmem,
            compiler_params=params,
            cost_estimate=pl.CostEstimate(
                flops=4 * cycles * tile * lanes, bytes_accessed=8 * cycles * tile * lanes, transcendentals=0
            ),
        )(position, *[pieces[distance] for distance in range(rows)])

    split_parts = [columns(pieces) for pieces in held]

    chunks = 2
    chunk = tile // chunks

    def dot(left, right):
        return lax.dot_general(
            left, right, (((1,), (1,)), ((), ())), preferred_element_type=jnp.float32
        )

    def multiply(position, *refs):
        own, blocks, refs = refs[:2], refs[2 : 2 + len(near)], refs[2 + len(near) :]
        columns_of = refs[:2]
        out, rows_of, stage, sems = refs[2:]
        row, col = position[0], position[1]
        own_turn = row // cols
        diagonal = row - own_turn * cols == col

        def copy(turn, part):
            where = slice(part * chunk, (part + 1) * chunk)
            return pltpu.make_async_copy(
                stage.at[turn, where], out.at[0, turn, 0, where], sems.at[turn, part]
            )

        wanted = [turn * cols + col <= row for turn in range(cycles)]
        for turn in range(cycles):

            @pl.when(jnp.logical_not(wanted[turn]))
            def _():
                stage[turn] = jnp.zeros((tile, tile), jnp.float32)
                for part in range(chunks):
                    copy(turn, part).start()

        @pl.when(diagonal)
        def _():
            for part in range(2):
                for place, kind in enumerate(ROW_ORDER):
                    first = COL_ORDER.index(kind) * lanes
                    rows_of[part, :, place * lanes : (place + 1) * lanes] = columns_of[part][
                        own_turn, :, first : first + lanes
                    ]

        @pl.when(jnp.logical_not(diagonal))
        def _():
            ahead = lax.rem(row, cols) < cols // 2
            for distance in range(cols):
                back = jnp.where(ahead, cols - distance, distance)
                start = lax.rem(col + back, cols) * depth
                for panel in range(panels):
                    source = blocks[distance - 1][panel] if distance else own[panel // half][panel % half]
                    if distance in halved:
                        source += blocks[cols - 3 + distance][panel]
                    split(source, rows_of, ROW_ORDER, panel // half, start, panel % half)

        for turn in range(cycles):

            @pl.when(wanted[turn])
            def _():
                for number in range(chunks):
                    where = slice(number * chunk, (number + 1) * chunk)
                    total = None
                    for part in range(2):
                        term = dot(rows_of[part, where], columns_of[part][turn])
                        term += dot(rows_of[part, where, :lanes], columns_of[part][turn, :, lanes:])
                        total = term if total is None else total + term
                    stage[turn, where] = total
                    copy(turn, number).start()

        for turn in range(cycles):
            for part in range(chunks):
                copy(turn, part).wait()

    half_rows = pltpu.VMEM((2, tile, len(ROW_ORDER) * lanes), jnp.bfloat16)
    return pl.pallas_call(
        multiply,
        out_shape=jax.ShapeDtypeStruct((1, cycles, 1, tile, tile), jnp.float32),
        in_specs=[smem] + [vmem] * (len(near) + 4),
        out_specs=pl.BlockSpec(memory_space=pl.ANY),
        scratch_shapes=[
            half_rows,
            pltpu.VMEM((cycles, tile, tile), jnp.float32),
            pltpu.SemaphoreType.DMA((cycles, chunks)),
        ],
        compiler_params=params,
        cost_estimate=pl.CostEstimate(
            flops=6 * cycles * tile * tile * panels * width,
            bytes_accessed=8 * cycles * tile * tile,
            transcendentals=0,
        ),
    )(position, *parts, *near, *split_parts)


def solution(mesh):
    in_specs = (P(None, ("row", "col"), None),)
    out_specs = P("row", None, "col", None, None)
    return jax.shard_map(tiles, mesh=mesh, in_specs=in_specs, out_specs=out_specs, check_vma=False)
```

```python
import jax
import jax.numpy as jnp
from jax import lax
from jax.experimental import pallas as pl
from jax.experimental.pallas import tpu as pltpu
from jax.sharding import PartitionSpec as P


ROW_ORDER, COL_ORDER = ("hi", "lo"), ("lo", "hi")


def swap(block, bits):
    count = lax.axis_size("row")
    route = [(low, low ^ bits) for low in range(count)]
    return lax.ppermute(block, "row", route)


def sense(row, cols):
    return 1 if row % cols < cols // 2 else -1


def reads(row, col, cols):
    return col < row and row % cols != col


def shift(block, distance, straight):
    rows, cols = lax.axis_size("row"), lax.axis_size("col")
    route = []
    for row in range(rows):
        for col in range(cols):
            place = col + sense(row, cols) * distance
            inside = 0 <= place < cols
            if straight in (None, inside) and (straight or reads(row, place % cols, cols)):
                route.append((row * cols + col, row * cols + place % cols))
    return lax.ppermute(block, ("row", "col"), route)


def transpose(block):
    rows, cols = lax.axis_size("row"), lax.axis_size("col")
    route = []
    for row in range(rows):
        for col in range(cols):
            target = row // cols * cols + (col + cols // 2) % cols
            route.append((row * cols + col, target * cols + row % cols))
    return lax.ppermute(block, ("row", "col"), route)


def row_bits(rows):
    bits = [1 << number for number in range(1, rows.bit_length() - 1)]
    distances = [0]
    for bit in bits:
        distances += [distance | bit for distance in distances]
    return distances[len(distances) // 2 :] + distances[1 : len(distances) // 2], 1


def tiles(jacobian):
    rows, cols = lax.axis_size("row"), lax.axis_size("col")
    cycles = rows // cols
    panels, depth, width = jacobian.shape
    tile = depth * cols
    half = panels // 2
    parts = (jacobian[:half], jacobian[half:])
    moved = [transpose(part) for part in parts]
    halved = range(2, cols - 1)
    near = [shift(jacobian, distance, True if distance in halved else None) for distance in range(1, cols)]
    near += [shift(jacobian, distance, False) for distance in halved]
    far, twin = row_bits(rows)
    held = []
    for part in moved:
        pieces = {0: part}
        for distance in far:
            pieces[distance] = swap(part, distance)
        for distance in [0] + far:
            pieces[distance ^ twin] = swap(pieces[distance], twin)
        held.append(pieces)
    vmem = pl.BlockSpec(memory_space=pltpu.VMEM)
    smem = pl.BlockSpec(memory_space=pltpu.SMEM)
    params = pltpu.CompilerParams(vmem_limit_bytes=16 << 20)
    lanes = half * width
    position = jnp.stack([lax.axis_index("row"), lax.axis_index("col")]).astype(jnp.int32)

    def split(value, parts, order, lead, start, panel):
        top = value.astype(jnp.bfloat16)
        rest = (value - top.astype(jnp.float32)).astype(jnp.bfloat16)
        where = pl.ds(pl.multiple_of(start, depth), depth)
        for place, kind in enumerate(order):
            first = place * lanes + panel * width
            parts[lead, where, first : first + width] = top if kind == "hi" else rest

    def split_columns(position, *refs):
        pieces, whole = refs[:rows], refs[rows]
        for distance, source in enumerate(pieces):
            holder = position[0] ^ distance
            turn = holder // cols
            slot = lax.rem(holder - turn * cols + cols - cols // 2, cols)
            for panel in range(half):
                split(source[panel], whole, COL_ORDER, turn, slot * depth, panel)

    def columns(pieces):
        shape = jax.ShapeDtypeStruct((cycles, tile, len(COL_ORDER) * lanes), jnp.bfloat16)
        return pl.pallas_call(
            split_columns,
            out_shape=shape,
            in_specs=[smem] + [vmem] * rows,
            out_specs=vmem,
            compiler_params=params,
            cost_estimate=pl.CostEstimate(
                flops=4 * cycles * tile * lanes, bytes_accessed=8 * cycles * tile * lanes, transcendentals=0
            ),
        )(position, *[pieces[distance] for distance in range(rows)])

    def split_row(position, distance, source, rows_of):
        back = jnp.where(lax.rem(position[0], cols) < cols // 2, cols - distance, distance)
        start = lax.rem(position[1] + back, cols) * depth
        for panel in range(panels):
            split(source(panel), rows_of, ROW_ORDER, panel // half, start, panel % half)

    def second_columns(position, *refs):
        split_row(position, 0, lambda panel: refs[panel // half][panel % half], refs[rows + 3])
        split_columns(position, *refs[2 : rows + 3])

    split_shape = jax.ShapeDtypeStruct((cycles, tile, len(COL_ORDER) * lanes), jnp.bfloat16)
    rows_shape = jax.ShapeDtypeStruct((2, tile, len(ROW_ORDER) * lanes), jnp.bfloat16)
    first_half = columns(held[0])
    second_half, own_rows = pl.pallas_call(
        second_columns,
        out_shape=(split_shape, rows_shape),
        in_specs=[smem] + [vmem] * (rows + 2),
        out_specs=(vmem, vmem),
        compiler_params=params,
        cost_estimate=pl.CostEstimate(
            flops=4 * cycles * tile * lanes, bytes_accessed=8 * cycles * tile * lanes, transcendentals=0
        ),
    )(position, *parts, *[held[1][distance] for distance in range(rows)])

    chunks = 2
    chunk = tile // chunks

    def dot(left, right):
        return lax.dot_general(
            left, right, (((1,), (1,)), ((), ())), preferred_element_type=jnp.float32
        )

    def multiply(position, *refs):
        blocks, refs = refs[: len(near)], refs[len(near) :]
        columns_of = refs[:2]
        out, rows_of, stage, sems = refs[3:]
        row, col = position[0], position[1]
        own_turn = row // cols
        diagonal = row - own_turn * cols == col

        def copy(turn, part):
            where = slice(part * chunk, (part + 1) * chunk)
            return pltpu.make_async_copy(
                stage.at[turn, where], out.at[0, turn, 0, where], sems.at[turn, part]
            )

        wanted = [turn * cols + col <= row for turn in range(cycles)]
        for turn in range(cycles):

            @pl.when(jnp.logical_not(wanted[turn]))
            def _():
                stage[turn] = jnp.zeros((tile, tile), jnp.float32)
                for part in range(chunks):
                    copy(turn, part).start()

        @pl.when(diagonal)
        def _():
            for part in range(2):
                for place, kind in enumerate(ROW_ORDER):
                    first = COL_ORDER.index(kind) * lanes
                    rows_of[part, :, place * lanes : (place + 1) * lanes] = columns_of[part][
                        own_turn, :, first : first + lanes
                    ]

        @pl.when(jnp.logical_not(diagonal))
        def _():
            for distance in range(1, cols):

                def source(panel):
                    value = blocks[distance - 1][panel]
                    if distance in halved:
                        value += blocks[cols - 3 + distance][panel]
                    return value

                split_row(position, distance, source, rows_of)

        for turn in range(cycles):

            @pl.when(wanted[turn])
            def _():
                for number in range(chunks):
                    where = slice(number * chunk, (number + 1) * chunk)
                    total = None
                    for part in range(2):
                        term = dot(rows_of[part, where], columns_of[part][turn])
                        term += dot(rows_of[part, where, :lanes], columns_of[part][turn, :, lanes:])
                        total = term if total is None else total + term
                    stage[turn, where] = total
                    copy(turn, number).start()

        for turn in range(cycles):
            for part in range(chunks):
                copy(turn, part).wait()

    return pl.pallas_call(
        multiply,
        out_shape=(jax.ShapeDtypeStruct((1, cycles, 1, tile, tile), jnp.float32), rows_shape),
        in_specs=[smem] + [vmem] * (len(near) + 3),
        out_specs=(pl.BlockSpec(memory_space=pl.ANY), vmem),
        input_output_aliases={len(near) + 3: 1},
        scratch_shapes=[
            pltpu.VMEM((cycles, tile, tile), jnp.float32),
            pltpu.SemaphoreType.DMA((cycles, chunks)),
        ],
        compiler_params=params,
        cost_estimate=pl.CostEstimate(
            flops=6 * cycles * tile * tile * panels * width,
            bytes_accessed=8 * cycles * tile * tile,
            transcendentals=0,
        ),
    )(position, *near, first_half, second_half, own_rows)[0]


def solution(mesh):
    in_specs = (P(None, ("row", "col"), None),)
    out_specs = P("row", None, "col", None, None)
    return jax.shard_map(tiles, mesh=mesh, in_specs=in_specs, out_specs=out_specs, check_vma=False)
```
